8 devices in a mesh: dp: 2 (over z, y), tp: 4 (over x, core).
Axes of the slice: x: 2, y: 2, z: 1, core: 2. Of those that a mesh axis runs over, the one named last changes fastest.
Arguments:
- x: bfloat16 [12, 2048, 3072], P('dp'), parts along dimension 0
- gamma: float32 [3072], replicated
- beta: float32 [3072], replicated
- wq: bfloat16 [3072, 4096], P(None, 'tp')
- wkv: bfloat16 [3072, 512], replicated
- wo: bfloat16 [4096, 3072], P('tp')
- w1: bfloat16 [3072, 24576], P(None, 'tp')
- w3: bfloat16 [3072, 24576], P(None, 'tp')
- w2: bfloat16 [24576, 3072], P('tp')
Outputs:
- output: bfloat16 [12, 2048, 3072], P('dp'), parts along dimension 0
There are 2 independent parts. The reference program is written for one: setup_inputs(seed, part) draws one part's arguments, and reference() takes and returns one part's arrays. A program takes and returns all parts, laid end to end along the dimension named above; an argument that names none is the same for every part.
All inputs are finite; a program needn't handle non-finite values.
Results may differ from the reference program's by a relative error of at most 0.0107695.
Values are sent between devices in bfloat16 or wider.
A program may use at most 1.25 GiB of HBM per device.

```python
import jax
import jax.numpy as jnp
from jax import lax
import math

D = 3072
HEADS = 16
HEAD = 256
FF = 24576
BATCH = 6
SEQ = 2048
EPS = 1e-5


def setup_inputs(seed: int = 0, part: int = 0) -> dict:
    key = jax.random.key(seed)
    ks = jax.random.split(key, 8)
    kx = jax.random.fold_in(jax.random.key(seed + 1), part)
    qscale = 0.85 * math.sqrt(max(1.0, math.log(SEQ / 32.0))) * D ** -0.5
    x = jax.random.normal(kx, (BATCH, SEQ, D), jnp.float32).astype(jnp.bfloat16)
    gamma = 1.0 + 0.3 * jax.random.normal(ks[0], (D,), jnp.float32)
    beta = 0.3 * jax.random.normal(ks[1], (D,), jnp.float32)
    wq = (qscale * jax.random.normal(ks[2], (D, HEADS * HEAD), jnp.float32)).astype(jnp.bfloat16)
    wkv = (D ** -0.5 * jax.random.normal(ks[3], (D, 2 * HEAD), jnp.float32)).astype(jnp.bfloat16)
    wo = (3.0 * (HEADS * HEAD) ** -0.5 * jax.random.normal(ks[4], (HEADS * HEAD, D), jnp.float32)).astype(jnp.bfloat16)
    w1 = (D ** -0.5 * jax.random.normal(ks[5], (D, FF), jnp.float32)).astype(jnp.bfloat16)
    w3 = (D ** -0.5 * jax.random.normal(ks[6], (D, FF), jnp.float32)).astype(jnp.bfloat16)
    w2 = (1.5 * FF ** -0.5 * jax.random.normal(ks[7], (FF, D), jnp.float32)).astype(jnp.bfloat16)
    return {'x': x, 'gamma': gamma, 'beta': beta, 'wq': wq, 'wkv': wkv, 'wo': wo, 'w1': w1, 'w3': w3, 'w2': w2}


def reference(x, gamma, beta, wq, wkv, wo, w1, w3, w2):
    qi = lax.broadcasted_iota(jnp.int32, (SEQ, SEQ), 0)
    ki = lax.broadcasted_iota(jnp.int32, (SEQ, SEQ), 1)
    causal = ki <= qi

    def one_seq(xs):
        xf = xs.astype(jnp.float32)
        mu = jnp.mean(xf, axis=-1, keepdims=True)
        var = jnp.mean(jnp.square(xf - mu), axis=-1, keepdims=True)
        ln = ((xf - mu) * lax.rsqrt(var + EPS) * gamma + beta).astype(jnp.bfloat16)
        q = jnp.dot(ln, wq, preferred_element_type=jnp.float32).astype(jnp.bfloat16)
        kv = jnp.dot(ln, wkv, preferred_element_type=jnp.float32).astype(jnp.bfloat16)
        k = kv[:, :HEAD]
        v = kv[:, HEAD:]

        def one_head(qh):
            s = jnp.dot(qh, k.T, preferred_element_type=jnp.float32) * HEAD ** -0.5
            s = jnp.where(causal, s, -1e30)
            p = jax.nn.softmax(s, axis=-1).astype(jnp.bfloat16)
            return jnp.dot(p, v, preferred_element_type=jnp.float32).astype(jnp.bfloat16)

        o = lax.map(one_head, q.reshape(SEQ, HEADS, HEAD).transpose(1, 0, 2))
        o = o.transpose(1, 0, 2).reshape(SEQ, HEADS * HEAD)
        a = jnp.dot(o, wo, preferred_element_type=jnp.float32)
        g = jnp.dot(ln, w1, preferred_element_type=jnp.float32)
        u = jnp.dot(ln, w3, preferred_element_type=jnp.float32)
        hm = (jax.nn.silu(g) * u).astype(jnp.bfloat16)
        m = jnp.dot(hm, w2, preferred_element_type=jnp.float32)
        return (xf + a + m).astype(jnp.bfloat16)

    return lax.map(one_seq, x)
```

```python
import functools

import jax
import jax.numpy as jnp
from jax import lax
from jax.experimental import pallas as pl
from jax.experimental.pallas import tpu as pltpu
from jax.sharding import PartitionSpec as P

EPS = 1e-5
LOG2E = 1.4426950408889634
BF = jnp.bfloat16
F32 = jnp.float32
RG = 16
VMEM_LIMIT = 63 * 2**20


def _params(n):
    return pltpu.CompilerParams(dimension_semantics=("arbitrary",) * n, vmem_limit_bytes=VMEM_LIMIT)


def _dot(a, b):
    return jnp.dot(a, b, preferred_element_type=F32)


def _cost(flops, nbytes):
    return pl.CostEstimate(flops=flops, bytes_accessed=nbytes, transcendentals=0)


def _qkv_kernel(x_ref, g_ref, b_ref, wq_ref, wkv_ref, ln_ref, q_ref, kv_ref, *, mc, nc):
    tm = x_ref.shape[0]
    rg = 16
    for r0 in range(0, tm, mc):
        for r in range(r0, r0 + mc, rg):
            xf = x_ref[r:r + rg, :].astype(F32)
            mu = jnp.mean(xf, axis=-1, keepdims=True)
            xc = xf - mu
            var = jnp.mean(xc * xc, axis=-1, keepdims=True)
            ln_ref[r:r + rg, :] = (xc * lax.rsqrt(var + EPS) * g_ref[...] + b_ref[...]).astype(BF)
        a = ln_ref[r0:r0 + mc, :]
        for w_ref, out_ref in ((wq_ref, q_ref), (wkv_ref, kv_ref)):
            for c in range(0, w_ref.shape[1], nc):
                out_ref[r0:r0 + mc, c:c + nc] = _dot(a, w_ref[:, c:c + nc]).astype(BF)


def _qkv(x, gamma, beta, wq, wkv, tm, mc, nc):
    t, d = x.shape
    nq, nkv = wq.shape[1], wkv.shape[1]
    row = lambda i: (i, 0)
    whole = lambda i: (0, 0)
    one = pl.Buffered(1)
    return pl.pallas_call(
        functools.partial(_qkv_kernel, mc=mc, nc=nc),
        grid=(t // tm,),
        in_specs=[pl.BlockSpec((tm, d), row), pl.BlockSpec((1, d), whole), pl.BlockSpec((1, d), whole),
                  pl.BlockSpec((d, nq), whole, pipeline_mode=one), pl.BlockSpec((d, nkv), whole, pipeline_mode=one)],
        out_specs=[pl.BlockSpec((tm, d), row), pl.BlockSpec((tm, nq), row), pl.BlockSpec((tm, nkv), row)],
        out_shape=[jax.ShapeDtypeStruct((t, d), BF), jax.ShapeDtypeStruct((t, nq), BF), jax.ShapeDtypeStruct((t, nkv), BF)],
        compiler_params=_params(1),
        cost_estimate=_cost(2 * t * d * (nq + nkv), 4 * t * d),
        name="qkv",
    )(x, gamma.reshape(1, d), beta.reshape(1, d), wq, wkv)


def _attn_kernel(q_ref, kv_ref, o_ref, *, seq, tq, dh, nh):
    i = pl.program_id(1)
    c2 = LOG2E * dh ** -0.5

    def block(c):
        end = (c + 1) * tq
        lo = end - tq
        row = lax.broadcasted_iota(jnp.int32, (tq, tq), 0)
        col = lax.broadcasted_iota(jnp.int32, (tq, tq), 1)
        for h in range(nh):
            q = q_ref[:, h * dh:(h + 1) * dh]
            s = lax.dot_general(q, kv_ref[:end, :dh], (((1,), (1,)), ((), ())), preferred_element_type=F32)
            sd = jnp.where(col <= row, s[:, lo:], -1e30)
            m = jnp.max(sd, axis=1, keepdims=True)
            if c:
                m = jnp.maximum(m, jnp.max(s[:, :lo], axis=1, keepdims=True))
            mc = m * c2
            p = jnp.exp2(sd * c2 - mc)
            l = jnp.sum(p, axis=1, keepdims=True)
            o = _dot(p.astype(BF), kv_ref[lo:end, dh:])
            if c:
                p = jnp.exp2(s[:, :lo] * c2 - mc)
                l = l + jnp.sum(p, axis=1, keepdims=True)
                o = o + _dot(p.astype(BF), kv_ref[:lo, dh:])
            o_ref[:, h * dh:(h + 1) * dh] = (o * (1.0 / l)).astype(BF)

    for c in range(seq // tq):
        @pl.when(i == c)
        def _(c=c):
            block(c)


def _attn(q, kv, seq, tq):
    t, w = q.shape
    dh = kv.shape[1] // 2
    nh = w // dh
    nq = seq // tq
    return pl.pallas_call(
        functools.partial(_attn_kernel, seq=seq, tq=tq, dh=dh, nh=nh),
        grid=(t // seq, nq),
        in_specs=[pl.BlockSpec((tq, w), lambda b, i: (b * nq + i, 0)), pl.BlockSpec((seq, 2 * dh), lambda b, i: (b, 0))],
        out_specs=pl.BlockSpec((tq, w), lambda b, i: (b * nq + i, 0)),
        out_shape=jax.ShapeDtypeStruct((t, w), BF),
        compiler_params=_params(2),
        cost_estimate=_cost(2 * t * seq * w, 4 * t * w),
        name="attn",
    )(q, kv)


def _mlp_kernel(x_hbm, ln_hbm, o_hbm, w1_hbm, w3_hbm, w2_hbm, wo_hbm, y_hbm,
                ln_v, o_v, h_v, wa, wb, wc, csy, pbuf, rbuf, xbuf, xin,
                wsem, lsem, osem, dsend, drecv, xsend, xrecv, xisem, ylsem, yssem, yrsem, *, nf, nn, tc):
    b, s = pl.program_id(0), pl.program_id(1)
    nb = pl.num_programs(0)
    ns = nf + nn
    np_ = 2 * nn
    tm, d = ln_v.shape
    hr = tm // 2
    me = lax.axis_index("tp")
    core = lax.rem(me, 2)
    other = {"tp": me + 1 - 2 * core}
    across = {"tp": lax.rem(me + 2, 4)}
    mesh_id = pl.DeviceIdType.MESH
    t = b * ns + s
    slot = lax.rem(t, 2)
    yb0 = 2 * np_ * hr

    def w_copies(step, sl):
        w = o_v.shape[1]
        at = pl.ds(sl * d, d)
        col = pl.ds(pl.multiple_of(step * (2 * tc), 2 * tc), 2 * tc)
        out1 = [(w1_hbm.at[:, col], wa.at[at], wsem.at[sl, 0]), (w3_hbm.at[:, col], wb.at[at], wsem.at[sl, 1])]
        col = pl.ds(pl.multiple_of((step - nf) * (2 * tc), 2 * tc), 2 * tc)
        out2 = [(w2_hbm.at[pl.ds(0, d), col], wa.at[at], wsem.at[sl, 0]), (w2_hbm.at[pl.ds(d, d), col], wb.at[at], wsem.at[sl, 1]),
                (wo_hbm.at[:, col], wc.at[pl.ds(sl * w, w)], wsem.at[sl, 2])]
        return out1, out2

    def w_do(step, sl, what):
        one, two = w_copies(step, sl)

        @pl.when(step < nf)
        def _():
            for c in one:
                getattr(pltpu.make_async_copy(*c), what)()

        @pl.when(step >= nf)
        def _():
            for c in two:
                getattr(pltpu.make_async_copy(*c), what)()

    def ln_copy(i):
        return pltpu.make_async_copy(ln_hbm.at[pl.ds(i * tm, tm)], ln_v, lsem)

    def o_copy(i):
        return pltpu.make_async_copy(o_hbm.at[pl.ds(i * tm, tm)], o_v, osem)

    def cs_at(par, i, r=0, n=hr):
        return pl.ds((par * np_ + i) * hr + r, n)

    def half_copy(blk, i):
        return pltpu.make_async_remote_copy(pbuf.at[i, 1 - core], rbuf.at[lax.rem(blk, 2), i], dsend.at[i],
                                            drecv.at[lax.rem(blk, 2), i], device_id=other, device_id_type=mesh_id)

    def sum_copy(blk, i):
        return pltpu.make_async_remote_copy(csy.at[cs_at(lax.rem(blk, 2), i)], xbuf.at[lax.rem(blk, 2), i], xsend.at[i],
                                            xrecv.at[lax.rem(blk, 2), i], device_id=across, device_id_type=mesh_id)

    def rows(k, c):
        blk, i = k // np_, lax.rem(k, np_)
        return (pl.ds(pl.multiple_of(blk * tm + c * hr, hr), hr), pl.ds(pl.multiple_of(i * tc, tc), tc))

    def x_copy(k):
        sl = lax.rem(k, 2)
        return pltpu.make_async_copy(x_hbm.at[rows(k, core)], xin.at[sl], xisem.at[sl])

    def y_rows(k):
        return csy.at[pl.ds(yb0 + lax.rem(k, 2) * hr, hr)]

    def y_local(k):
        return pltpu.make_async_copy(y_rows(k), y_hbm.at[rows(k, core)], ylsem.at[lax.rem(k, 2)])

    def y_remote(k):
        blk, i = k // np_, lax.rem(k, np_)
        return pltpu.make_async_remote_copy(y_rows(k), y_hbm.at[rows(k, core)], yssem.at[lax.rem(k, 2)],
                                            yrsem.at[lax.rem(blk, 2), i], device_id=other, device_id_type=mesh_id)

    def y_arrival(k):
        blk, i = k // np_, lax.rem(k, np_)
        return pltpu.make_async_remote_copy(y_rows(k), y_hbm.at[rows(k, 1 - core)], yssem.at[lax.rem(k, 2)],
                                            yrsem.at[lax.rem(blk, 2), i], device_id=other, device_id_type=mesh_id)

    def cs_wait(blk, i):
        half_copy(blk, i).wait_recv()
        half_copy(blk, i).wait_send()

    def cs_add(par, i):
        for r in range(0, hr, RG):
            at = pl.ds(r, RG)
            csy[cs_at(par, i, r, RG), :] = (pbuf[i, core, at].astype(F32) + rbuf[par, i, at].astype(F32)).astype(BF)

    def y_wait(k):
        blk, i = k // np_, lax.rem(k, np_)
        sum_copy(blk, i).wait_recv()
        sum_copy(blk, i).wait_send()
        x_copy(k).wait()

        @pl.when(k >= 2)
        def _():
            y_local(k - 2).wait()
            y_remote(k - 2).wait_send()

        @pl.when(k >= np_)
        def _():
            y_arrival(k - np_).wait_recv()

    def y_add(par, i, sl):
        for r in range(0, hr, RG):
            at = pl.ds(r, RG)
            both = csy[cs_at(par, i, r, RG), :].astype(F32) + xbuf[par, i, at].astype(F32)
            csy[pl.ds(yb0 + sl * hr + r, RG), :] = (xin[sl, at].astype(F32) + both).astype(BF)

    def y_write(k):
        y_local(k).start()
        y_remote(k).start()

    @pl.when(t == 0)
    def _():
        barrier = pltpu.get_barrier_semaphore()
        for dev in (other, across):
            pl.semaphore_signal(barrier, inc=1, device_id=dev, device_id_type=mesh_id)
        pl.semaphore_wait(barrier, 2)
        w_do(s, slot, "start")
        ln_copy(b).start()
        x_copy(0).start()

    @pl.when(t < nb * ns - 1)
    def _():
        w_do(lax.rem(s + 1, ns), 1 - slot, "start")

    @pl.when(s == 0)
    def _():
        o_copy(b).start()
        ln_copy(b).wait()

    @pl.when(s == nf)
    def _():
        o_copy(b).wait()

        @pl.when(b < nb - 1)
        def _():
            ln_copy(b + 1).start()

    w_do(s, slot, "wait")

    @pl.when(s < nf)
    def _():
        k = np_ * b + s - (np_ + 3)

        @pl.when(b >= 1)
        def _():
            cs_wait(b - 1, s)

        @pl.when(k >= 0)
        def _():
            y_wait(k)

        cs_add(lax.rem(b + 1, 2), s)
        y_add(jnp.where(k >= 0, lax.rem(k // np_, 2), 1), lax.rem(s + 3, np_), jnp.where(k >= 0, lax.rem(k, 2), 1))
        for sub in range(2):
            at, cl = pl.ds(slot * d, d), pl.ds(sub * tc, tc)
            g = _dot(ln_v[...], wa[at, cl])
            u = _dot(ln_v[...], wb[at, cl])
            h_v[:, pl.ds(pl.multiple_of((s * 2 + sub) * tc, tc), tc)] = (g * jax.nn.sigmoid(g) * u).astype(BF)

        @pl.when(b >= 1)
        def _():
            sum_copy(b - 1, s).start()

        @pl.when(k >= 0)
        def _():
            y_write(k)
            x_copy(k + 1).start()

    @pl.when(s >= nf)
    def _():
        p = s - nf

        @pl.when((b == nb - 1) & (p >= 1))
        def _():
            for j in range(2):
                i = 2 * (p - 1) + j
                cs_wait(b, i)
                cs_add(lax.rem(b, 2), i)
                sum_copy(b, i).start()

        for sub in range(2):
            at, cl = pl.ds(slot * d, d), pl.ds(sub * tc, tc)
            w = o_v.shape[1]
            part = (_dot(h_v[:, :d], wa[at, cl]) + _dot(h_v[:, d:], wb[at, cl])
                    + _dot(o_v[...], wc[pl.ds(slot * w, w), cl])).astype(BF)
            for c in range(2):
                pbuf[2 * p + sub, c] = part[c * hr:(c + 1) * hr]
        for sub in range(2):
            half_copy(b, 2 * p + sub).start()

    @pl.when(t == nb * ns - 1)
    def _():
        for i in range(np_ - 2, np_):
            cs_wait(b, i)
            cs_add(lax.rem(b, 2), i)
            sum_copy(b, i).start()

        def finish(k, carry):
            y_wait(k)
            y_add(lax.rem(k // np_, 2), lax.rem(k, np_), lax.rem(k, 2))
            y_write(k)

            @pl.when(k + 1 < np_ * nb)
            def _():
                x_copy(k + 1).start()
            return carry

        last = np_ * nb
        lax.fori_loop(last - np_ - 3, last, finish, 0)
        for k in (last - 2, last - 1):
            y_local(k).wait()
            y_remote(k).wait_send()

        def drain(k, carry):
            y_arrival(k).wait_recv()
            return carry

        lax.fori_loop(last - np_, last, drain, 0)


def _mlp(x, ln, o, w1, w3, w2, wo, tm, tc):
    t, d = x.shape
    f, w = w1.shape[1], o.shape[1]
    nf, nn = f // (2 * tc), d // (2 * tc)
    assert nf == 2 * nn and f == 2 * d
    nb = t // tm
    np_, hr = 2 * nn, tm // 2
    hbm = pl.BlockSpec(memory_space=pltpu.HBM)
    dma = pltpu.SemaphoreType.DMA
    return pl.pallas_call(
        functools.partial(_mlp_kernel, nf=nf, nn=nn, tc=tc),
        grid=(nb, nf + nn),
        in_specs=[hbm] * 7,
        out_specs=hbm,
        out_shape=jax.ShapeDtypeStruct((t, d), BF),
        scratch_shapes=[pltpu.VMEM((tm, d), BF), pltpu.VMEM((tm, w), BF), pltpu.VMEM((tm, f), BF),
                        pltpu.VMEM((2 * d, 2 * tc), BF), pltpu.VMEM((2 * d, 2 * tc), BF), pltpu.VMEM((2 * w, 2 * tc), BF), pltpu.VMEM(((2 * np_ + 2) * hr, tc), BF),
                        pltpu.VMEM((np_, 2, hr, tc), BF), pltpu.VMEM((2, np_, hr, tc), BF), pltpu.VMEM((2, np_, hr, tc), BF),
                        pltpu.VMEM((2, hr, tc), BF),
                        dma((2, 3)), dma(()), dma(()), dma((np_,)), dma((2, np_)), dma((np_,)), dma((2, np_)),
                        dma((2,)), dma((2,)), dma((2,)), dma((2, np_))],
        compiler_params=pltpu.CompilerParams(dimension_semantics=("arbitrary",) * 2, vmem_limit_bytes=VMEM_LIMIT,
                                             collective_id=0, has_side_effects=True),
        cost_estimate=_cost(2 * t * (3 * d * f + d * w), 2 * t * (3 * d + w) + 6 * d * f * nb),
        name="mlp",
    )(x, ln, o, w1, w3, w2, wo)


def solution(mesh):
    def local(x, gamma, beta, wq, wkv, wo, w1, w3, w2):
        b, s, d = x.shape
        t = b * s
        xt = x.reshape(t, d)
        ln, q, kv = _qkv(xt, gamma, beta, wq, wkv, 512, 128, 512)
        o = _attn(q, kv, s, 512)
        return _mlp(xt, ln, o, w1, w3, w2, wo, 512, d // 6).reshape(b, s, d)

    return jax.shard_map(local, mesh=mesh,
                         in_specs=(P('dp', None, None), P(), P(), P(None, 'tp'), P(), P('tp', None),
                                   P(None, 'tp'), P(None, 'tp'), P('tp', None)),
                         out_specs=P('dp', None, None), check_vma=False)
```

```python
import functools

import jax
import jax.numpy as jnp
from jax import lax
from jax.experimental import pallas as pl
from jax.experimental.pallas import tpu as pltpu
from jax.sharding import PartitionSpec as P

EPS = 1e-5
LOG2E = 1.4426950408889634
BF = jnp.bfloat16
F32 = jnp.float32
VMEM_LIMIT = 63 * 2**20


def _params(n):
    return pltpu.CompilerParams(dimension_semantics=("arbitrary",) * n, vmem_limit_bytes=VMEM_LIMIT)


def _dot(a, b):
    return jnp.dot(a, b, preferred_element_type=F32)


def _cost(flops, nbytes):
    return pl.CostEstimate(flops=flops, bytes_accessed=nbytes, transcendentals=0)


def _qkv_kernel(x_ref, g_ref, b_ref, wq_ref, wkv_ref, ln_ref, q_ref, kv_ref, *, mc, nc):
    tm = x_ref.shape[0]
    rg = 16
    for r0 in range(0, tm, mc):
        for r in range(r0, r0 + mc, rg):
            xf = x_ref[r:r + rg, :].astype(F32)
            mu = jnp.mean(xf, axis=-1, keepdims=True)
            xc = xf - mu
            var = jnp.mean(xc * xc, axis=-1, keepdims=True)
            ln_ref[r:r + rg, :] = (xc * lax.rsqrt(var + EPS) * g_ref[...] + b_ref[...]).astype(BF)
        a = ln_ref[r0:r0 + mc, :]
        for w_ref, out_ref in ((wq_ref, q_ref), (wkv_ref, kv_ref)):
            for c in range(0, w_ref.shape[1], nc):
                out_ref[r0:r0 + mc, c:c + nc] = _dot(a, w_ref[:, c:c + nc]).astype(BF)


def _qkv(x, gamma, beta, wq, wkv, tm, mc, nc):
    t, d = x.shape
    nq, nkv = wq.shape[1], wkv.shape[1]
    row = lambda i: (i, 0)
    whole = lambda i: (0, 0)
    one = pl.Buffered(1)
    return pl.pallas_call(
        functools.partial(_qkv_kernel, mc=mc, nc=nc),
        grid=(t // tm,),
        in_specs=[pl.BlockSpec((tm, d), row), pl.BlockSpec((1, d), whole), pl.BlockSpec((1, d), whole),
                  pl.BlockSpec((d, nq), whole, pipeline_mode=one), pl.BlockSpec((d, nkv), whole, pipeline_mode=one)],
        out_specs=[pl.BlockSpec((tm, d), row), pl.BlockSpec((tm, nq), row), pl.BlockSpec((tm, nkv), row)],
        out_shape=[jax.ShapeDtypeStruct((t, d), BF), jax.ShapeDtypeStruct((t, nq), BF), jax.ShapeDtypeStruct((t, nkv), BF)],
        compiler_params=_params(1),
        cost_estimate=_cost(2 * t * d * (nq + nkv), 4 * t * d),
        name="qkv",
    )(x, gamma.reshape(1, d), beta.reshape(1, d), wq, wkv)


def _attn_kernel(q_ref, kv_ref, o_ref, *, seq, tq, dh, nh):
    i = pl.program_id(1)
    c2 = LOG2E * dh ** -0.5

    def block(c):
        end = (c + 1) * tq
        lo = end - tq
        row = lax.broadcasted_iota(jnp.int32, (tq, tq), 0)
        col = lax.broadcasted_iota(jnp.int32, (tq, tq), 1)
        for h in range(nh):
            q = q_ref[:, h * dh:(h + 1) * dh]
            s = lax.dot_general(q, kv_ref[:end, :dh], (((1,), (1,)), ((), ())), preferred_element_type=F32)
            sd = jnp.where(col <= row, s[:, lo:], -1e30)
            m = jnp.max(sd, axis=1, keepdims=True)
            if c:
                m = jnp.maximum(m, jnp.max(s[:, :lo], axis=1, keepdims=True))
            mc = m * c2
            p = jnp.exp2(sd * c2 - mc)
            l = jnp.sum(p, axis=1, keepdims=True)
            o = _dot(p.astype(BF), kv_ref[lo:end, dh:])
            if c:
                p = jnp.exp2(s[:, :lo] * c2 - mc)
                l = l + jnp.sum(p, axis=1, keepdims=True)
                o = o + _dot(p.astype(BF), kv_ref[:lo, dh:])
            o_ref[:, h * dh:(h + 1) * dh] = (o * (1.0 / l)).astype(BF)

    for c in range(seq // tq):
        @pl.when(i == c)
        def _(c=c):
            block(c)


def _attn(q, kv, seq, tq):
    t, w = q.shape
    dh = kv.shape[1] // 2
    nh = w // dh
    nq = seq // tq
    return pl.pallas_call(
        functools.partial(_attn_kernel, seq=seq, tq=tq, dh=dh, nh=nh),
        grid=(t // seq, nq),
        in_specs=[pl.BlockSpec((tq, w), lambda b, i: (b * nq + i, 0)), pl.BlockSpec((seq, 2 * dh), lambda b, i: (b, 0))],
        out_specs=pl.BlockSpec((tq, w), lambda b, i: (b * nq + i, 0)),
        out_shape=jax.ShapeDtypeStruct((t, w), BF),
        compiler_params=_params(2),
        cost_estimate=_cost(2 * t * seq * w, 4 * t * w),
        name="attn",
    )(q, kv)


SLOTS = 4
RG = 16


def _mlp_kernel(x_hbm, ln_hbm, o_hbm, w1_hbm, w3_hbm, w2_hbm, wo_hbm, y_hbm,
                ln_v, o_v, h_v, wa, wb, wc, csy, pbuf, rbuf, xbuf, xin,
                wsem, lsem, osem, dsend, drecv, xsend, xrecv, xisem, ylsem, yssem, yrsem, *, nf, nn, uf, un):
    b, s = pl.program_id(0), pl.program_id(1)
    nb = pl.num_programs(0)
    sf = nf // uf
    last_step = sf + nn // un - 1
    tm, d = ln_v.shape
    w = o_v.shape[1]
    tc = wa.shape[1]
    hr = tm // 2
    me = lax.axis_index("tp")
    core = lax.rem(me, 2)
    other = {"tp": me + 1 - 2 * core}
    across = {"tp": lax.rem(me + 2, 4)}
    mesh_id = pl.DeviceIdType.MESH
    ncol = nf + nn
    yb0 = 2 * nn * hr

    def w_copies(g, j, kind):
        sl = lax.rem(g, SLOTS)
        at = pl.ds(sl * d, d)
        if kind == 0:
            col = pl.ds(pl.multiple_of(j * tc, tc), tc)
            todo = [(w1_hbm.at[:, col], wa.at[at]), (w3_hbm.at[:, col], wb.at[at])]
        else:
            col = pl.ds(pl.multiple_of((j - nf) * tc, tc), tc)
            todo = [(w2_hbm.at[pl.ds(0, d), col], wa.at[at]), (w2_hbm.at[pl.ds(d, d), col], wb.at[at]),
                    (wo_hbm.at[:, col], wc.at[pl.ds(sl * w, w)])]
        return [pltpu.make_async_copy(src, dst, wsem.at[sl, i]) for i, (src, dst) in enumerate(todo)]

    def w_wait(g, j, kind):
        for c in w_copies(g, j, kind):
            c.wait()

    def w_start(g):
        j = lax.rem(g, ncol)
        for kind in range(2):
            @pl.when((g < nb * ncol) & ((j < nf) if kind == 0 else (j >= nf)))
            def _(kind=kind):
                for c in w_copies(g, j, kind):
                    c.start()

    def ln_copy(i):
        return pltpu.make_async_copy(ln_hbm.at[pl.ds(i * tm, tm)], ln_v, lsem)

    def o_copy(i):
        return pltpu.make_async_copy(o_hbm.at[pl.ds(i * tm, tm)], o_v, osem)

    def cs_at(par, i, r=0, n=hr):
        return pl.ds((par * nn + i) * hr + r, n)

    def half_copy(blk, i):
        return pltpu.make_async_remote_copy(pbuf.at[i, 1 - core], rbuf.at[lax.rem(blk, 2), i], dsend.at[i],
                                            drecv.at[lax.rem(blk, 2), i], device_id=other, device_id_type=mesh_id)

    def sum_copy(blk, i):
        return pltpu.make_async_remote_copy(csy.at[cs_at(lax.rem(blk, 2), i)], xbuf.at[lax.rem(blk, 2), i], xsend.at[i],
                                            xrecv.at[lax.rem(blk, 2), i], device_id=across, device_id_type=mesh_id)

    def rows(k, c):
        blk, i = k // nn, lax.rem(k, nn)
        return (pl.ds(pl.multiple_of(blk * tm + c * hr, hr), hr), pl.ds(pl.multiple_of(i * tc, tc), tc))

    def x_copy(k):
        sl = lax.rem(k, 2)
        return pltpu.make_async_copy(x_hbm.at[rows(k, core)], xin.at[sl], xisem.at[sl])

    def y_rows(k):
        return csy.at[pl.ds(yb0 + lax.rem(k, 2) * hr, hr)]

    def y_local(k):
        return pltpu.make_async_copy(y_rows(k), y_hbm.at[rows(k, core)], ylsem.at[lax.rem(k, 2)])

    def y_remote(k, c):
        blk, i = k // nn, lax.rem(k, nn)
        return pltpu.make_async_remote_copy(y_rows(k), y_hbm.at[rows(k, c)], yssem.at[lax.rem(k, 2)],
                                            yrsem.at[lax.rem(blk, 2), i], device_id=other, device_id_type=mesh_id)

    def cs_wait(blk, i):
        half_copy(blk, i).wait_recv()
        half_copy(blk, i).wait_send()

    def cs_add(par, i):
        for r in range(0, hr, RG):
            at = pl.ds(r, RG)
            csy[cs_at(par, i, r, RG), :] = (pbuf[i, core, at].astype(F32) + rbuf[par, i, at].astype(F32)).astype(BF)

    def y_wait(k):
        blk, i = k // nn, lax.rem(k, nn)
        sum_copy(blk, i).wait_recv()
        sum_copy(blk, i).wait_send()
        x_copy(k).wait()

        @pl.when(k >= 2)
        def _():
            y_local(k - 2).wait()
            y_remote(k - 2, core).wait_send()

        @pl.when(k >= nn)
        def _():
            y_remote(k - nn, 1 - core).wait_recv()

    def y_add(par, i, sl):
        for r in range(0, hr, RG):
            at = pl.ds(r, RG)
            both = csy[cs_at(par, i, r, RG), :].astype(F32) + xbuf[par, i, at].astype(F32)
            csy[pl.ds(yb0 + sl * hr + r, RG), :] = (xin[sl, at].astype(F32) + both).astype(BF)

    def y_write(k):
        y_local(k).start()
        y_remote(k, core).start()

        @pl.when(k + 1 < nn * nb)
        def _():
            x_copy(k + 1).start()

    @pl.when((b == 0) & (s == 0))
    def _():
        barrier = pltpu.get_barrier_semaphore()
        for dev in (other, across):
            pl.semaphore_signal(barrier, inc=1, device_id=dev, device_id_type=mesh_id)
        pl.semaphore_wait(barrier, 2)
        for g in range(SLOTS - 1):
            w_start(jnp.int32(g))
        ln_copy(b).start()
        x_copy(0).start()

    @pl.when(s == 0)
    def _():
        o_copy(b).start()
        ln_copy(b).wait()

    @pl.when(s == sf)
    def _():
        o_copy(b).wait()

        @pl.when(b < nb - 1)
        def _():
            ln_copy(b + 1).start()

    k = nn * b + s - nn - 2

    @pl.when(b >= 1)
    def _():
        cs_wait(b - 1, s)

    @pl.when(k >= 0)
    def _():
        y_wait(k)

    def sums():
        cs_add(lax.rem(b + 1, 2), s)
        y_add(jnp.where(k >= 0, lax.rem(k // nn, 2), 1), lax.rem(s + nn - 2, nn), jnp.where(k >= 0, lax.rem(k, 2), 1))

    def early_sums(items):
        for i in items:
            cs_wait(b, i)
            cs_add(lax.rem(b, 2), i)
            sum_copy(b, i).start()

    @pl.when(s < sf)
    def _():
        j0 = s * uf
        g0 = b * ncol + j0
        for u in range(uf):
            w_wait(g0 + u, j0 + u, 0)
        sums()
        for u in range(uf):
            w_start(g0 + u + SLOTS - 1)
            at = pl.ds(lax.rem(g0 + u, SLOTS) * d, d)
            gate = _dot(ln_v[...], wa[at, :])
            up = _dot(ln_v[...], wb[at, :])
            h_v[:, pl.ds(pl.multiple_of((j0 + u) * tc, tc), tc)] = (gate * jax.nn.sigmoid(gate) * up).astype(BF)

    @pl.when(s >= sf)
    def _():
        n0 = (s - sf) * un
        g0 = b * ncol + nf + n0

        @pl.when((b == nb - 1) & (s == last_step))
        def _():
            early_sums(range(nn - un))

        for u in range(un):
            w_wait(g0 + u, nf + n0 + u, 1)
        sums()
        for u in range(un):
            w_start(g0 + u + SLOTS - 1)
            sl = lax.rem(g0 + u, SLOTS)
            at = pl.ds(sl * d, d)
            part = (_dot(h_v[:, :d], wa[at, :]) + _dot(h_v[:, d:], wb[at, :])
                    + _dot(o_v[...], wc[pl.ds(sl * w, w), :])).astype(BF)
            for c in range(2):
                pbuf[n0 + u, c] = part[c * hr:(c + 1) * hr]
        for u in range(un):
            half_copy(b, n0 + u).start()

    @pl.when(b >= 1)
    def _():
        sum_copy(b - 1, s).start()

    @pl.when(k >= 0)
    def _():
        y_write(k)

    @pl.when((b == nb - 1) & (s == last_step))
    def _():
        last = nn * nb

        def finish(k, carry):
            y_wait(k)
            y_add(lax.rem(k // nn, 2), lax.rem(k, nn), lax.rem(k, 2))
            y_write(k)
            return carry

        early_sums(range(nn - un, nn))
        lax.fori_loop(last - nn - 2, last, finish, 0)
        for k in (last - 2, last - 1):
            y_local(k).wait()
            y_remote(k, core).wait_send()

        def drain(k, carry):
            y_remote(k, 1 - core).wait_recv()
            return carry

        lax.fori_loop(last - nn, last, drain, 0)


def _mlp(x, ln, o, w1, w3, w2, wo, tm, tc, uf, un):
    t, d = x.shape
    f, w = w1.shape[1], o.shape[1]
    nf, nn = f // tc, d // tc
    nb = t // tm
    hr = tm // 2
    assert f == 2 * d and nf // uf + nn // un == nn and nf % uf == 0 and nn % un == 0
    hbm = pl.BlockSpec(memory_space=pltpu.HBM)
    dma = pltpu.SemaphoreType.DMA
    return pl.pallas_call(
        functools.partial(_mlp_kernel, nf=nf, nn=nn, uf=uf, un=un),
        grid=(nb, nf // uf + nn // un),
        in_specs=[hbm] * 7,
        out_specs=hbm,
        out_shape=jax.ShapeDtypeStruct((t, d), BF),
        scratch_shapes=[pltpu.VMEM((tm, d), BF), pltpu.VMEM((tm, w), BF), pltpu.VMEM((tm, f), BF),
                        pltpu.VMEM((SLOTS * d, tc), BF), pltpu.VMEM((SLOTS * d, tc), BF), pltpu.VMEM((SLOTS * w, tc), BF),
                        pltpu.VMEM(((2 * nn + 2) * hr, tc), BF),
                        pltpu.VMEM((nn, 2, hr, tc), BF), pltpu.VMEM((2, nn, hr, tc), BF), pltpu.VMEM((2, nn, hr, tc), BF),
                        pltpu.VMEM((2, hr, tc), BF),
                        dma((SLOTS, 3)), dma(()), dma(()), dma((nn,)), dma((2, nn)), dma((nn,)), dma((2, nn)),
                        dma((2,)), dma((2,)), dma((2,)), dma((2, nn))],
        compiler_params=pltpu.CompilerParams(dimension_semantics=("arbitrary",) * 2, vmem_limit_bytes=VMEM_LIMIT,
                                             collective_id=0, has_side_effects=True),
        cost_estimate=_cost(2 * t * (3 * d * f + d * w), 2 * t * (3 * d + w) + 6 * d * f * nb),
        name="mlp",
    )(x, ln, o, w1, w3, w2, wo)


def solution(mesh):
    def local(x, gamma, beta, wq, wkv, wo, w1, w3, w2):
        b, s, d = x.shape
        t = b * s
        xt = x.reshape(t, d)
        ln, q, kv = _qkv(xt, gamma, beta, wq, wkv, 512, 128, 512)
        o = _attn(q, kv, s, 512)
        return _mlp(xt, ln, o, w1, w3, w2, wo, 512, d // 6, 3, 3).reshape(b, s, d)

    return jax.shard_map(local, mesh=mesh,
                         in_specs=(P('dp', None, None), P(), P(), P(None, 'tp'), P(), P('tp', None),
                                   P(None, 'tp'), P(None, 'tp'), P('tp', None)),
                         out_specs=P('dp', None, None), check_vma=False)
```

```python
import functools

import jax
import jax.numpy as jnp
from jax import lax
from jax.experimental import pallas as pl
from jax.experimental.pallas import tpu as pltpu
from jax.sharding import PartitionSpec as P

EPS = 1e-5
LOG2E = 1.4426950408889634
BF = jnp.bfloat16
F32 = jnp.float32
VMEM_LIMIT = 67043328


def _params(n):
    return pltpu.CompilerParams(dimension_semantics=("arbitrary",) * n, vmem_limit_bytes=VMEM_LIMIT)


def _dot(a, b):
    return jnp.dot(a, b, preferred_element_type=F32)


def _cost(flops, nbytes):
    return pl.CostEstimate(flops=flops, bytes_accessed=nbytes, transcendentals=0)


def _qkv_kernel(x_ref, g_ref, b_ref, wq_ref, wkv_ref, ln_ref, q_ref, kv_ref, *, mc, nc):
    tm = x_ref.shape[0]
    rg = 16
    for r0 in range(0, tm, mc):
        for r in range(r0, r0 + mc, rg):
            xf = x_ref[r:r + rg, :].astype(F32)
            mu = jnp.mean(xf, axis=-1, keepdims=True)
            xc = xf - mu
            var = jnp.mean(xc * xc, axis=-1, keepdims=True)
            ln_ref[r:r + rg, :] = (xc * lax.rsqrt(var + EPS) * g_ref[...] + b_ref[...]).astype(BF)
        a = ln_ref[r0:r0 + mc, :]
        for w_ref, out_ref in ((wq_ref, q_ref), (wkv_ref, kv_ref)):
            for c in range(0, w_ref.shape[1], nc):
                out_ref[r0:r0 + mc, c:c + nc] = _dot(a, w_ref[:, c:c + nc]).astype(BF)


def _qkv(x, gamma, beta, wq, wkv, tm, mc, nc):
    t, d = x.shape
    nq, nkv = wq.shape[1], wkv.shape[1]
    row = lambda i: (i, 0)
    whole = lambda i: (0, 0)
    one = pl.Buffered(1)
    return pl.pallas_call(
        functools.partial(_qkv_kernel, mc=mc, nc=nc),
        grid=(t // tm,),
        in_specs=[pl.BlockSpec((tm, d), row), pl.BlockSpec((1, d), whole), pl.BlockSpec((1, d), whole),
                  pl.BlockSpec((d, nq), whole, pipeline_mode=one), pl.BlockSpec((d, nkv), whole, pipeline_mode=one)],
        out_specs=[pl.BlockSpec((tm, d), row), pl.BlockSpec((tm, nq), row), pl.BlockSpec((tm, nkv), row)],
        out_shape=[jax.ShapeDtypeStruct((t, d), BF), jax.ShapeDtypeStruct((t, nq), BF), jax.ShapeDtypeStruct((t, nkv), BF)],
        compiler_params=_params(1),
        cost_estimate=_cost(2 * t * d * (nq + nkv), 4 * t * d),
        name="qkv",
    )(x, gamma.reshape(1, d), beta.reshape(1, d), wq, wkv)


def _attn_kernel(q_ref, kv_ref, o_ref, *, seq, tq, dh, nh):
    i = pl.program_id(1)
    c2 = LOG2E * dh ** -0.5

    def block(c):
        end = (c + 1) * tq
        lo = end - tq
        row = lax.broadcasted_iota(jnp.int32, (tq, tq), 0)
        col = lax.broadcasted_iota(jnp.int32, (tq, tq), 1)
        for h in range(nh):
            q = q_ref[:, h * dh:(h + 1) * dh]
            s = lax.dot_general(q, kv_ref[:end, :dh], (((1,), (1,)), ((), ())), preferred_element_type=F32)
            sd = jnp.where(col <= row, s[:, lo:], -1e30)
            m = jnp.max(sd, axis=1, keepdims=True)
            if c:
                m = jnp.maximum(m, jnp.max(s[:, :lo], axis=1, keepdims=True))
            mc = m * c2
            p = jnp.exp2(sd * c2 - mc)
            l = jnp.sum(p, axis=1, keepdims=True)
            o = _dot(p.astype(BF), kv_ref[lo:end, dh:])
            if c:
                p = jnp.exp2(s[:, :lo] * c2 - mc)
                l = l + jnp.sum(p, axis=1, keepdims=True)
                o = o + _dot(p.astype(BF), kv_ref[:lo, dh:])
            o_ref[:, h * dh:(h + 1) * dh] = (o * (1.0 / l)).astype(BF)

    for c in range(seq // tq):
        @pl.when(i == c)
        def _(c=c):
            block(c)


def _attn(q, kv, seq, tq):
    t, w = q.shape
    dh = kv.shape[1] // 2
    nh = w // dh
    nq = seq // tq
    return pl.pallas_call(
        functools.partial(_attn_kernel, seq=seq, tq=tq, dh=dh, nh=nh),
        grid=(t // seq, nq),
        in_specs=[pl.BlockSpec((tq, w), lambda b, i: (b * nq + i, 0)), pl.BlockSpec((seq, 2 * dh), lambda b, i: (b, 0))],
        out_specs=pl.BlockSpec((tq, w), lambda b, i: (b * nq + i, 0)),
        out_shape=jax.ShapeDtypeStruct((t, w), BF),
        compiler_params=_params(2),
        cost_estimate=_cost(2 * t * seq * w, 4 * t * w),
        name="attn",
    )(q, kv)


SLOTS = 3
RG = 32


def _mlp_kernel(x_hbm, ln_hbm, o_hbm, w1_hbm, w3_hbm, w2_hbm, wo_hbm, y_hbm,
                ln_v, o_v, h_v, gate_v, wa, wb, wc, csum, yrow, pieces, rbuf, xbuf, xin,
                wsem, lsem, osem, dsend, drecv, xsend, xrecv, xisem, ylsem, yssem, yrsem, rfree, xfree, *, nf, nn):
    b, s = pl.program_id(0), pl.program_id(1)
    nb = pl.num_programs(0)
    sf, sn = nf // 2, nn // 2
    last_step = sf + sn - 1
    tm, d = ln_v.shape
    w = o_v.shape[1]
    tc = wa.shape[1]
    hr = tm // 2
    lag = nn // 2
    me = lax.axis_index("tp")
    core = lax.rem(me, 2)
    other = {"tp": me + 1 - 2 * core}
    across = {"tp": lax.rem(me + 2, 4)}
    mesh_id = pl.DeviceIdType.MESH
    ncol = nf + nn

    def w_copies(g, j, kind):
        sl = lax.rem(g, SLOTS)
        at = pl.ds(sl * d, d)
        if kind == 0:
            col = pl.ds(pl.multiple_of(j * tc, tc), tc)
            todo = [(w1_hbm.at[:, col], wa.at[at]), (w3_hbm.at[:, col], wb.at[at])]
        else:
            col = pl.ds(pl.multiple_of((j - nf) * tc, tc), tc)
            todo = [(w2_hbm.at[pl.ds(0, d), col], wa.at[at]), (w2_hbm.at[pl.ds(d, d), col], wb.at[at]),
                    (wo_hbm.at[:, col], wc.at[pl.ds(sl * w, w)])]
        return [pltpu.make_async_copy(src, dst, wsem.at[sl, i]) for i, (src, dst) in enumerate(todo)]

    def w_wait(g, j, kind):
        for c in w_copies(g, j, kind):
            c.wait()

    def w_start(g):
        j = lax.rem(g, ncol)
        for kind in range(2):
            @pl.when((g < nb * ncol) & ((j < nf) if kind == 0 else (j >= nf)))
            def _(kind=kind):
                for c in w_copies(g, j, kind):
                    c.start()

    def ln_copy(i):
        return pltpu.make_async_copy(ln_hbm.at[pl.ds(i * tm, tm)], ln_v, lsem)

    def o_copy(i):
        return pltpu.make_async_copy(o_hbm.at[pl.ds(i * tm, tm)], o_v, osem)

    def half_copy(i):
        return pltpu.make_async_remote_copy(pieces.at[nn + lax.rem(i, 2)], rbuf.at[i], dsend.at[i], drecv.at[i],
                                            device_id=other, device_id_type=mesh_id)

    def sum_copy(i):
        return pltpu.make_async_remote_copy(csum.at[i], xbuf.at[i], xsend.at[i], xrecv.at[i],
                                            device_id=across, device_id_type=mesh_id)

    def rows(k, c):
        blk, i = k // nn, lax.rem(k, nn)
        return (pl.ds(pl.multiple_of(blk * tm + c * hr, hr), hr), pl.ds(pl.multiple_of(i * tc, tc), tc))

    def x_copy(k):
        return pltpu.make_async_copy(x_hbm.at[rows(k, core)], xin.at[0], xisem)

    def y_local(k):
        return pltpu.make_async_copy(yrow.at[0], y_hbm.at[rows(k, core)], ylsem)

    def y_remote(k, c):
        return pltpu.make_async_remote_copy(yrow.at[0], y_hbm.at[rows(k, c)], yssem,
                                            yrsem.at[lax.rem(k // nn, 2), lax.rem(k, nn)], device_id=other, device_id_type=mesh_id)

    def half_start(blk, i):
        @pl.when(blk >= 1)
        def _():
            pl.semaphore_wait(rfree.at[i], 1)
        half_copy(i).start()

    def cs_wait(i):
        half_copy(i).wait_recv()

        @pl.when(i >= nn - 2)
        def _():
            half_copy(i).wait_send()

    def groups(body, rolled):
        if rolled:
            @pl.loop(0, hr // RG)
            def _(r):
                body(pl.ds(pl.multiple_of(r * RG, RG), RG))
        else:
            for r in range(0, hr, RG):
                body(pl.ds(r, RG))

    def cs_add(i, r_at, rolled=False):
        def body(at):
            csum[i, at] = (pieces[i, at].astype(F32) + rbuf[r_at, at].astype(F32)).astype(BF)

        groups(body, rolled)

    def cs_send(blk, i):
        @pl.when(blk < nb - 1)
        def _():
            pl.semaphore_signal(rfree.at[i], inc=1, device_id=other, device_id_type=mesh_id)

        @pl.when(blk >= 1)
        def _():
            pl.semaphore_wait(xfree.at[i], 1)
        sum_copy(i).start()

    def y_wait(k):
        i = lax.rem(k, nn)
        sum_copy(i).wait_recv()
        sum_copy(i).wait_send()
        x_copy(k).wait()

        @pl.when(k >= 1)
        def _():
            y_local(k - 1).wait()
            y_remote(k - 1, core).wait_send()

        @pl.when(k >= nn)
        def _():
            y_remote(k - nn, 1 - core).wait_recv()

    def y_add(i, x_at, rolled=False):
        def body(at):
            both = csum[i, at].astype(F32) + xbuf[x_at, at].astype(F32)
            yrow[0, at] = (xin[0, at].astype(F32) + both).astype(BF)

        groups(body, rolled)

    def y_write(k):
        @pl.when(k < nn * (nb - 1))
        def _():
            pl.semaphore_signal(xfree.at[lax.rem(k, nn)], inc=1, device_id=across, device_id_type=mesh_id)
        y_local(k).start()
        y_remote(k, core).start()

    def y_all(k):
        y_wait(k)
        y_add(lax.rem(k, nn), lax.rem(k, nn), rolled=True)
        y_write(k)

        @pl.when(k + 1 < nn * nb)
        def _():
            x_copy(k + 1).start()

    def cs_all(i):
        cs_wait(i)
        cs_add(i, i, rolled=True)
        cs_send(b, i)

    @pl.when((b == 0) & (s == 0))
    def _():
        barrier = pltpu.get_barrier_semaphore()
        for dev in (other, across):
            pl.semaphore_signal(barrier, inc=1, device_id=dev, device_id_type=mesh_id)
        pl.semaphore_wait(barrier, 2)
        for g in range(SLOTS - 1):
            w_start(jnp.int32(g))
        ln_copy(b).start()

    @pl.when(s == 0)
    def _():
        o_copy(b).start()
        ln_copy(b).wait()

    @pl.when(s == sf)
    def _():
        o_copy(b).wait()

        @pl.when(b < nb - 1)
        def _():
            ln_copy(b + 1).start()

    @pl.when(s < sf)
    def _():
        j0 = 2 * s
        g0 = b * ncol + j0
        k = nn * b + s - nn - lag

        @pl.when(b >= 1)
        def _():
            cs_wait(s)

        @pl.when(k >= 0)
        def _():
            y_wait(k)

        for u in range(2):
            w_wait(g0 + u, j0 + u, 0)
        cs_add(s, jnp.where(b >= 1, s, nn))
        i = lax.rem(s + nn - lag, nn)
        y_add(i, jnp.where(k >= 0, i, nn))
        for u in range(2):
            w_start(g0 + u + SLOTS - 1)
            at = pl.ds(lax.rem(g0 + u, SLOTS) * d, d)
            gate_v[...] = _dot(ln_v[...], wa[at, :])
            up = _dot(ln_v[...], wb[at, :])
            gate = gate_v[...]
            h_v[:, pl.ds(pl.multiple_of((j0 + u) * tc, tc), tc)] = (gate * jax.nn.sigmoid(gate) * up).astype(BF)

        @pl.when(b >= 1)
        def _():
            cs_send(b - 1, s)

        @pl.when(k >= 0)
        def _():
            y_write(k)

        @pl.when(k >= -1)
        def _():
            x_copy(k + 1).start()

    @pl.when(s >= sf)
    def _():
        n0 = 2 * (s - sf)
        g0 = b * ncol + nf + n0

        @pl.when((b == nb - 1) & (s > sf))
        def _():
            def old(k, carry):
                y_all(k)
                return carry

            first = nn * (b - 1) + nn - lag
            lax.fori_loop(first + (s - sf - 1) * (lag - 1), jnp.minimum(first + (s - sf) * (lag - 1), nn * b), old, 0)

            @pl.loop(n0 - 2, n0)
            def _(i):
                cs_all(i)

        @pl.when(s > sf)
        def _():
            for u in range(2):
                half_copy(n0 - 2 + u).wait_send()

        for u in range(2):
            w_wait(g0 + u, nf + n0 + u, 1)
        for u in range(2):
            w_start(g0 + u + SLOTS - 1)
            sl = lax.rem(g0 + u, SLOTS)
            at = pl.ds(sl * d, d)
            part = (_dot(h_v[:, :d], wa[at, :]) + _dot(h_v[:, d:], wb[at, :])
                    + _dot(o_v[...], wc[pl.ds(sl * w, w), :])).astype(BF)
            for c in range(2):
                pieces[jnp.where(core == c, n0 + u, nn + u)] = part[c * hr:(c + 1) * hr]
        for u in range(2):
            half_start(b, n0 + u)

    @pl.when((b == nb - 1) & (s == last_step))
    def _():
        last = nn * nb

        @pl.loop(nn - 2, nn)
        def _(i):
            cs_all(i)

        def finish(k, carry):
            y_all(k)
            return carry

        lax.fori_loop(last - nn, last, finish, 0)
        y_local(last - 1).wait()
        y_remote(last - 1, core).wait_send()

        def drain(k, carry):
            y_remote(k, 1 - core).wait_recv()
            return carry

        lax.fori_loop(last - nn, last, drain, 0)


def _mlp(x, ln, o, w1, w3, w2, wo, tm, tc):
    t, d = x.shape
    f, w = w1.shape[1], o.shape[1]
    nf, nn = f // tc, d // tc
    nb = t // tm
    hr = tm // 2
    assert f == 2 * d and nn == 6
    hbm = pl.BlockSpec(memory_space=pltpu.HBM)
    dma = pltpu.SemaphoreType.DMA
    half = lambda n: pltpu.VMEM((n, hr, tc), BF)
    return pl.pallas_call(
        functools.partial(_mlp_kernel, nf=nf, nn=nn),
        grid=(nb, (nf + nn) // 2),
        in_specs=[hbm] * 7,
        out_specs=hbm,
        out_shape=jax.ShapeDtypeStruct((t, d), BF),
        scratch_shapes=[pltpu.VMEM((tm, d), BF), pltpu.VMEM((tm, w), BF), pltpu.VMEM((tm, f), BF), pltpu.VMEM((tm, tc), F32),
                        pltpu.VMEM((SLOTS * d, tc), BF), pltpu.VMEM((SLOTS * d, tc), BF), pltpu.VMEM((SLOTS * w, tc), BF),
                        half(nn), half(1), half(nn + 2), half(nn + 1), half(nn + 1), half(1),
                        dma((SLOTS, 3)), dma(()), dma(()), dma((nn,)), dma((nn,)), dma((nn,)), dma((nn,)),
                        dma(()), dma(()), dma(()), dma((2, nn)),
                        pltpu.SemaphoreType.REGULAR((nn,)), pltpu.SemaphoreType.REGULAR((nn,))],
        compiler_params=pltpu.CompilerParams(dimension_semantics=("arbitrary",) * 2, vmem_limit_bytes=VMEM_LIMIT,
                                             collective_id=0, has_side_effects=True),
        cost_estimate=_cost(2 * t * (3 * d * f + d * w), 2 * t * (3 * d + w) + 6 * d * f * nb),
        name="mlp",
    )(x, ln, o, w1, w3, w2, wo)


def solution(mesh):
    def local(x, gamma, beta, wq, wkv, wo, w1, w3, w2):
        b, s, d = x.shape
        t = b * s
        xt = x.reshape(t, d)
        ln, q, kv = _qkv(xt, gamma, beta, wq, wkv, 384, 128, 512)
        o = _attn(q, kv, s, 512)
        return _mlp(xt, ln, o, w1, w3, w2, wo, 1024, d // 6).reshape(b, s, d)

    return jax.shard_map(local, mesh=mesh,
                         in_specs=(P('dp', None, None), P(), P(), P(None, 'tp'), P(), P('tp', None),
                                   P(None, 'tp'), P(None, 'tp'), P('tp', None)),
                         out_specs=P('dp', None, None), check_vma=False)
```
